256 devices in a mesh: grp: 4 (over x_hi, core), ep: 64 (over z, x_lo, y).
Axes of the slice: x: 4 (x_hi: 2, x_lo: 2; x = x_hi * 2 + x_lo), y: 4, z: 8, core: 2. Of those that a mesh axis runs over, the one named last changes fastest.
Arguments:
- features: bfloat16 [65536, 1152], P(('grp', 'ep')), may hold values from -6 to 6
- token_position: int32 [65536], P(('grp', 'ep')), may hold values from 0 to 16383, as said below
- expert_ids: int32 [65536, 2], P(('grp', 'ep')), may hold values from 0 to 63, all different within a row; in each aligned block of 256 rows (0 to 255, 256 to 511, ...) at most 16 rows name the same one
- proj_in: bfloat16 [1152, 2560], P('ep'), may hold values from -0.1875 to 0.1875
- bias_in: float32 [2560], replicated, may hold values from -3 to 3
- proj_out: bfloat16 [2560, 2560], P('ep'), may hold values from -0.125 to 0.125
- bias_out: float32 [2560], replicated, may hold values from -3 to 3
- norm_gain: float32 [2560], replicated, may hold values from 0.1 to 1.9
- router: bfloat16 [2560, 64], replicated, may hold values from -0.125 to 0.125
- w_gate: bfloat16 [64, 2560, 512], P('ep'), may hold values from -0.125 to 0.125
- w_up: bfloat16 [64, 2560, 512], P('ep'), may hold values from -0.125 to 0.125
- w_down: bfloat16 [64, 512, 2560], P('ep'), may hold values from -0.25 to 0.25
Outputs:
- mixed: bfloat16 [65536, 2560], P(('grp', 'ep'))
The draws below stay inside these ranges and needn't reach their ends.
Inputs may be any that keep to these rules, and one draw needn't show every extreme that they name: `token_position`: within each group of 64 devices along ep, the group's values form a permutation of 0 to 16383; position q belongs to the device of ep index q // 256. The rows of each device hold exactly 4 positions of every device of its group. `expert_ids`: each row names 2 different experts; no expert is named by more than 16 of the rows of one device.
All inputs are finite; a program needn't handle non-finite values.
Results may differ from the reference program's by a relative error of at most 0.0071.
Values may be sent and summed in bfloat16 or wider, within the bound.
No kernel may reach another device: no remote copies, remote signals or barrier semaphores. Data moves between devices by JAX's collectives and lax.ppermute only.
A program may use at most 192 MiB of HBM per device.

```python
import math
import jax
import jax.numpy as jnp
import numpy as np
from jax import lax

D_VIS = 1152
D = 2560
FF_E = 512
TOP = 2
EXP_DEV = 1
ROWS = 256
EXPERTS = 64
CAP = 16
ROWS_ALL = 65536
N_GRP = 4
N_EP = 64


def group_positions(group_key):
    first_key, second_key = jax.random.split(group_key)
    per_peer = ROWS // N_EP
    template = jnp.repeat(jnp.arange(N_EP, dtype=jnp.int32), per_peer)

    def shuffle_template(single_key):
        return jax.random.permutation(single_key, template)

    def shuffle_rows(single_key):
        return jax.random.permutation(single_key, ROWS).astype(jnp.int32)
    destinations = jax.vmap(shuffle_template)(jax.random.split(first_key, N_EP))
    dest_hot = (destinations[:, :, None] == jnp.arange(N_EP, dtype=jnp.int32)[None, None, :]).astype(jnp.int32)
    ranking = jnp.sum((jnp.cumsum(dest_hot, axis=1) - 1) * dest_hot, axis=2)
    canonical = jnp.arange(N_EP, dtype=jnp.int32)[:, None] * per_peer + ranking
    shuffles = jax.vmap(shuffle_rows)(jax.random.split(second_key, N_EP))
    landing = shuffles[destinations, canonical]
    return (destinations * ROWS + landing).reshape(N_EP * ROWS).astype(jnp.int32)


def draw_token_position(key, part):
    group_keys = jax.random.split(jax.random.fold_in(key, 17), N_GRP)
    return jax.vmap(group_positions)(group_keys).reshape(N_GRP * N_EP * ROWS)


def shard_levels(rng, shape, pieces, smallest, top_value):
    def one(dim, blocks):
        heights = jax.random.uniform(jax.random.fold_in(jax.random.fold_in(rng, 6), dim), (blocks,), jnp.float32, smallest / len(pieces), top_value / len(pieces))
        return jnp.repeat(jnp.exp(heights), shape[dim] // blocks).reshape((-1,) + (1,) * (len(shape) - dim - 1))

    level = one(*pieces[0])
    for cut in pieces[1:]:
        level = level * one(*cut)
    return level


def deal_out(own_key, own, number, rows, number_of, top, bound, skew):
    sequence = jax.random.permutation(own_key, number_of)
    packed, common = load_shares(number_of, rows * top, bound, skew, True), load_shares(number_of, rows * top, bound, skew, False)
    places = jnp.arange(number_of)

    def named(tallies, offset_by):
        used = int((tallies > 0).sum())
        fixed = max(1, used // 4)
        moved = fixed + (places - fixed + offset_by * (used - fixed)) % max(1, number_of - fixed)
        return jnp.zeros((number_of,), jnp.int32).at[sequence[jnp.where(places < fixed, places, moved)]].set(jnp.asarray(tallies, jnp.int32))

    tallies = jnp.where(number % 4 == 0, named(packed, number // 4), named(common, number - number // 4 - 1))
    mixed = jax.random.permutation(jax.random.fold_in(own, 3), number_of)
    donor, taker = mixed[0:number_of // 2 * 2:2], mixed[1:number_of // 2 * 2:2]
    margin = jnp.minimum(tallies[donor] - 1, bound - tallies[taker]) // 2
    margin = jnp.where((donor == sequence[0]) | (taker == sequence[0]) | (tallies[taker] == 0), 0, jnp.maximum(margin, 0))
    moved = jax.random.randint(jax.random.fold_in(own, 4), (number_of // 2,), 0, 1 << 20) % (margin + 1)
    tallies = tallies.at[donor].add(-moved).at[taker].add(moved)
    labels = jnp.searchsorted(jnp.cumsum(tallies), jnp.arange(rows * top), side="right").astype(jnp.int32)
    grid = labels.reshape(top, rows).T
    grid = grid[jax.random.permutation(jax.random.fold_in(own, 1), rows)]
    offset_by = jax.random.randint(jax.random.fold_in(own, 2), (rows, 1), 0, top)
    return jnp.take_along_axis(grid, (jnp.arange(top)[None, :] + offset_by) % top, axis=1)


def load_shares(count, total, bound, slope, full):
    loads = [(1 << 20) // math.isqrt(rank ** slope) + 1 for rank in range(1, count + 1)]
    largest = bound if full else min(bound, max(-(-total // count), total * loads[0] // sum(loads)))
    least = 1 if total - largest >= count - 1 else 0
    counts, surplus = [largest] + [least] * (count - 1), total - largest - least * (count - 1)
    while surplus > 0:
        movable = [i for i in range(1, count) if counts[i] < largest] or [i for i in range(1, count) if counts[i] < bound]
        whole, left = sum([loads[i] for i in movable]), surplus
        for i in movable:
            addition = min(bound - counts[i], max(1, left * loads[i] // whole), surplus)
            counts[i] = counts[i] + addition
            surplus = surplus - addition
    return np.array(counts)


def centred(key, extent, spread, reach, cuts=(), kind=jnp.bfloat16):
    loudness = shard_levels(key, extent, cuts, -0.22, 0.18) if cuts else 1.0
    entries = jax.random.normal(key, extent, jnp.float32) * spread * loudness
    return jnp.minimum(jnp.maximum(entries, -reach), reach).astype(kind)


def setup_inputs(seed: int = 0) -> dict:
    arg_keys = jax.random.split(jax.random.key(seed), 13)
    features = centred(arg_keys[0], (ROWS_ALL, D_VIS), 1.0, 6.0, ((0, 256),))
    token_position = draw_token_position(jax.random.fold_in(arg_keys[12], 71), 0)
    expert_ids_keys = jax.random.split(jax.random.fold_in(arg_keys[2], 1), ROWS_ALL // ROWS)
    expert_ids_turns = jax.random.permutation(jax.random.fold_in(arg_keys[2], 3), ROWS_ALL // ROWS)
    expert_ids = jax.vmap(lambda own, number: deal_out(jax.random.fold_in(arg_keys[2], 2), own, number, ROWS, EXPERTS, TOP, CAP, 2))(expert_ids_keys, expert_ids_turns).reshape((ROWS_ALL, TOP))
    proj_in = centred(arg_keys[3], (D_VIS, D), D_VIS ** -0.5, 0.1875, ((0, 64),))
    bias_in = centred(arg_keys[4], (D,), 0.5, 3.0, (), jnp.float32)
    proj_out = centred(arg_keys[5], (D, D), D ** -0.5, 0.125, ((0, 64),))
    bias_out = centred(arg_keys[6], (D,), 0.5, 3.0, (), jnp.float32)
    norm_gain = jnp.clip(1.0 + 0.18 * jax.random.normal(arg_keys[7], (D,), jnp.float32), 0.1, 1.9)
    router = centred(arg_keys[8], (D, EXPERTS), D ** -0.5, 0.125)
    w_gate = centred(arg_keys[9], (EXPERTS, D, FF_E), D ** -0.5, 0.125, ((0, 64),))
    w_up = centred(arg_keys[10], (EXPERTS, D, FF_E), D ** -0.5, 0.125, ((0, 64),))
    w_down = centred(arg_keys[11], (EXPERTS, FF_E, D), FF_E ** -0.5, 0.25, ((0, 64),))
    return {"features": features, "token_position": token_position, "expert_ids": expert_ids, "proj_in": proj_in, "bias_in": bias_in, "proj_out": proj_out, "bias_out": bias_out, "norm_gain": norm_gain, "router": router, "w_gate": w_gate, "w_up": w_up, "w_down": w_down}


EPSILON = 1e-06

def run_expert(operands):
    rows_in, gate_weight, up_weight, down_weight = operands
    gate_part = jnp.dot(rows_in, gate_weight, preferred_element_type=jnp.float32)
    up_part = jnp.dot(rows_in, up_weight, preferred_element_type=jnp.float32)
    activated = (jax.nn.silu(gate_part) * up_part).astype(jnp.bfloat16)
    return jnp.dot(activated, down_weight, preferred_element_type=jnp.float32).astype(jnp.bfloat16)

def reference(features, token_position, expert_ids, proj_in, bias_in, proj_out, bias_out, norm_gain, router, w_gate, w_up, w_down):
    group_rows = N_EP * ROWS
    experts = EXP_DEV * N_EP
    capacity = 2 * ROWS * TOP // experts

    def one_group(group_index):
        offset = (group_index * group_rows).astype(jnp.int32)
        patches = lax.dynamic_slice_in_dim(features, offset, group_rows, 0)
        positions = lax.dynamic_slice_in_dim(token_position, offset, group_rows, 0)
        choices = lax.dynamic_slice_in_dim(expert_ids, offset, group_rows, 0)
        pre_act = jnp.dot(patches, proj_in, preferred_element_type=jnp.float32) + bias_in
        hidden = jax.nn.gelu(pre_act, approximate=False).astype(jnp.bfloat16)
        projected = (jnp.dot(hidden, proj_out, preferred_element_type=jnp.float32) + bias_out).astype(jnp.bfloat16)
        tokens = jnp.zeros_like(projected).at[positions].set(projected)
        wide = tokens.astype(jnp.float32)
        scale = lax.rsqrt(lax.optimization_barrier(jnp.mean(wide * wide, axis=-1, keepdims=True)) + EPSILON)
        normed = (wide * scale * norm_gain).astype(jnp.bfloat16)
        logits = jnp.dot(normed, router, preferred_element_type=jnp.float32)
        chosen_mask = choices[:, :, None] == jnp.arange(experts, dtype=jnp.int32)[None, None, :]
        chosen = lax.optimization_barrier(jnp.sum(jnp.where(chosen_mask, logits[:, None, :], 0.0), axis=2))
        first_gate = jax.nn.sigmoid(chosen[:, 0] - chosen[:, 1])
        gates = jnp.stack([first_gate, 1.0 - first_gate], axis=1)
        pair_expert = choices.reshape(N_EP, ROWS * TOP)
        pair_hot = (pair_expert[:, :, None] == jnp.arange(experts, dtype=jnp.int32)[None, None, :]).astype(jnp.int32)
        pair_slot = lax.optimization_barrier(jnp.sum((jnp.cumsum(pair_hot, axis=1) - 1) * pair_hot, axis=2)).astype(jnp.int32)
        device_index = jnp.broadcast_to(jnp.arange(N_EP, dtype=jnp.int32)[:, None], (N_EP, ROWS * TOP))
        pair_rows = jnp.repeat(normed, TOP, axis=0).reshape(N_EP, ROWS * TOP, D)
        blocks = jnp.zeros((experts, N_EP, capacity, D), jnp.bfloat16).at[pair_expert, device_index, pair_slot].set(pair_rows)
        outputs = lax.map(run_expert, (blocks.reshape(experts, N_EP * capacity, D), w_gate, w_up, w_down))
        outputs = outputs.reshape(experts, N_EP, capacity, D)
        combined = outputs[pair_expert, device_index, pair_slot].reshape(group_rows, TOP, D)
        total = wide + lax.optimization_barrier(jnp.sum(gates[:, :, None] * combined.astype(jnp.float32), axis=1))
        return total.astype(jnp.bfloat16)
    results = lax.map(one_group, jnp.arange(N_GRP, dtype=jnp.int32))
    return results.reshape(N_GRP * group_rows, D)
```

```python
import functools

import jax
import jax.numpy as jnp
from jax import lax
from jax.experimental import pallas as pl
from jax.experimental.pallas import tpu as pltpu
from jax.sharding import Mesh, PartitionSpec as P

EPSILON = 1e-06
BF = jnp.bfloat16
F32 = jnp.float32
I32 = jnp.int32

XH, CO, Z, XL, Y = 2, 2, 8, 2, 4
ALL = ("xh", "co", "z", "xl", "y")
EP = ("z", "xl", "y")
D_VIS, D, FF = 1152, 2560, 512
ROWS, EXPERTS, CAP = 256, 64, 16
HALF = CAP // 2
SLOTS = EXPERTS * HALF
R_IN, R_OUT = D_VIS // EXPERTS, D // EXPERTS
COLUMNS = XL * Y
C_IN, C_OUT = R_IN * Z, R_OUT * Z
PIECE = 64
BLOCK = C_IN + C_OUT
QUARTERS = XH * CO
QW = D // QUARTERS
GATHERED = XH * XL * Y * CO
SEND_W = D_VIS + 128
TILE = 256


def iota(shape, dim):
    return lax.broadcasted_iota(I32, shape, dim)


def hot(mask):
    return jnp.where(mask, 1.0, 0.0).astype(BF)


def divided(x, by):
    return jnp.floor((x.astype(F32) + 0.5) * (1.0 / by)).astype(I32)


def product(a, b):
    return jnp.dot(a, b, preferred_element_type=F32)


def vmem():
    return pl.BlockSpec(memory_space=pltpu.VMEM)


def smem():
    return pl.BlockSpec(memory_space=pltpu.SMEM)


def hbm():
    return pl.BlockSpec(memory_space=pl.ANY)


def call(body, outs, in_specs, out_specs, scratch=(), flops=0, limit=48, name=None):
    return pl.pallas_call(
        body,
        out_shape=outs,
        in_specs=in_specs,
        out_specs=out_specs,
        scratch_shapes=list(scratch),
        name=name,
        cost_estimate=pl.CostEstimate(flops=flops, bytes_accessed=1 << 20, transcendentals=0),
        compiler_params=pltpu.CompilerParams(vmem_limit_bytes=limit << 20),
    )


def piece_body(quarter, w_in, w_out, piece):
    q = quarter[0]
    new = iota((1, QW), 1) + q * QW
    col = divided(new, C_OUT)
    rest = new - col * C_OUT
    z = divided(rest, R_OUT)
    old = z * (COLUMNS * R_OUT) + col * R_OUT + (rest - z * R_OUT)
    order = hot(iota((D, QW), 0) == old)
    picked = product(w_in[...], order).astype(BF)
    piece[0:R_OUT, :] = w_out[:, pl.ds(pl.multiple_of(q * QW, 128), QW)]
    piece[R_OUT : R_OUT + R_IN, :] = picked
    piece[R_OUT + R_IN : PIECE, :] = jnp.zeros((PIECE - R_OUT - R_IN, QW), BF)


def pack_body(own_z, *refs):
    pieces, out = refs[:-1], refs[-1]
    k = iota((1, PIECE), 1)
    row = iota((BLOCK, PIECE), 0)
    total = jnp.zeros((BLOCK, QW), F32)
    for d in range(Z):
        source = lax.rem(own_z[0] + (Z - d), Z)
        first = source * R_OUT + k
        second = C_OUT + source * R_IN + (k - R_OUT)
        target = jnp.where(k < R_OUT, first, jnp.where(k < R_OUT + R_IN, second, -1))
        total = total + product(hot(row == target), pieces[d][...])
    out[...] = total.astype(BF)


def send_body(position, features, out):
    pos = position[...].astype(F32)
    wide = jnp.broadcast_to(pos, (ROWS, ROWS))
    earlier = jnp.where(wide.T < wide, 1.0, 0.0)
    rank = jnp.sum(earlier, axis=0, keepdims=True)
    picks = iota((ROWS, ROWS), 0).astype(F32) == rank
    landing = pos - jnp.floor(pos * (1.0 / ROWS)) * ROWS
    landed = jnp.sum(jnp.where(picks, jnp.broadcast_to(landing, (ROWS, ROWS)), 0.0), axis=1, keepdims=True)
    ordered = product(hot(picks), features[...]).astype(BF)
    new = iota((1, D_VIS), 1)
    col = divided(new, C_IN)
    rest = new - col * C_IN
    z = divided(rest, R_IN)
    old = z * (COLUMNS * R_IN) + col * R_IN + (rest - z * R_IN)
    order = hot(iota((D_VIS, D_VIS), 0) == old)
    out[:, 0:D_VIS] = product(ordered, order).astype(BF)
    out[:, D_VIS:SEND_W] = jnp.broadcast_to(landed, (ROWS, SEND_W - D_VIS)).astype(BF)


def place_body(received, ids_t, own, blocks):
    landing = received[:, D_VIS:SEND_W].astype(F32).T[0:1, :]
    place = hot(iota((ROWS, ROWS), 0).astype(F32) == landing)
    tokens = product(place, received[:, 0:D_VIS]).astype(BF)
    own[...] = tokens
    expert = iota((EXPERTS, ROWS), 0)
    named = (expert == ids_t[0:1, :]) | (expert == ids_t[1:2, :])
    before = hot(iota((ROWS, ROWS), 0) < iota((ROWS, ROWS), 1))
    count = product(hot(named), before)
    slot = jnp.where(named, count, -1.0).astype(BF)
    spread = hot((iota((SLOTS, EXPERTS), 0) >> 3) == iota((SLOTS, EXPERTS), 1))
    slots = product(spread, slot)
    within = (iota((SLOTS, ROWS), 0) & 7).astype(F32)
    for half in range(2):
        chosen = hot(slots == within + float(half * HALF))
        blocks[:, half * D_VIS : (half + 1) * D_VIS] = product(chosen, tokens).astype(BF)


def weight_copies(gathered, w_a, w_b, sems):
    first, second = [], []
    for b in range(GATHERED):
        xh, xl, y, co = b // (XL * Y * CO), b // (Y * CO) % XL, b // CO % Y, b % CO
        column, quarter = xl * Y + y, xh * CO + co
        cols = pl.ds(quarter * QW, QW)
        first.append(
            pltpu.make_async_copy(
                gathered.at[pl.ds(b * BLOCK + C_OUT, C_IN), :],
                w_a.at[pl.ds(column * C_IN, C_IN), cols],
                sems.at[b],
            )
        )
        second.append(
            pltpu.make_async_copy(
                gathered.at[pl.ds(b * BLOCK, C_OUT), :],
                w_b.at[pl.ds(column * C_OUT, C_OUT), cols],
                sems.at[GATHERED + b],
            )
        )
    return first, second


def projector(x, w_a, w_b, bias_in, bias_out, hidden, tokens, squares, first, second):
    for copy in first:
        copy.wait()

    def up(n, carry):
        cols = pl.ds(pl.multiple_of(n * TILE, TILE), TILE)
        pre = product(x[...], w_a[:, cols]) + bias_in[:, cols]
        hidden[:, cols] = (0.5 * pre * (1.0 + lax.erf(pre * 0.7071067811865476))).astype(BF)
        return carry

    lax.fori_loop(0, D // TILE, up, 0, unroll=2)
    for copy in second:
        copy.wait()
    squares[...] = jnp.zeros(squares.shape, F32)

    def down(n, carry):
        cols = pl.ds(pl.multiple_of(n * TILE, TILE), TILE)
        result = (product(hidden[...], w_b[:, cols]) + bias_out[:, cols]).astype(BF)
        tokens[:, cols] = result
        wide = result.astype(F32)
        wide = wide * wide
        squares[...] += wide[:, 0:128] + wide[:, 128:256]
        return carry

    lax.fori_loop(0, D // TILE, down, 0, unroll=2)
    mean = jnp.sum(squares[...], axis=1, keepdims=True) * (1.0 / D)
    return lax.rsqrt(mean + EPSILON)


def normalise(tokens, scale, gain, normed):
    def one(n, carry):
        cols = pl.ds(pl.multiple_of(n * TILE, TILE), TILE)
        normed[:, cols] = (tokens[:, cols].astype(F32) * scale * gain[:, cols]).astype(BF)
        return carry

    lax.fori_loop(0, D // TILE, one, 0)


def expert_body(
    x, gathered, bias_in, bias_out, gain, w_gate, w_up, w_down, out,
    w_a, w_b, g_ref, u_ref, d_ref, hidden, tokens, act, squares, sems,
):
    first, second = weight_copies(gathered, w_a, w_b, sems)
    base = 2 * GATHERED
    third = [
        pltpu.make_async_copy(w_gate.at[0], g_ref, sems.at[base]),
        pltpu.make_async_copy(w_up.at[0], u_ref, sems.at[base + 1]),
        pltpu.make_async_copy(w_down.at[0], d_ref, sems.at[base + 2]),
    ]
    for copy in first + second + third:
        copy.start()
    scale = projector(x, w_a, w_b, bias_in, bias_out, hidden, tokens, squares, first, second)
    normalise(tokens, scale, gain, hidden)
    for copy in third:
        copy.wait()

    def gated(n, carry):
        cols = pl.ds(pl.multiple_of(n * TILE, TILE), TILE)
        gate = product(hidden[...], g_ref[:, cols])
        up = product(hidden[...], u_ref[:, cols])
        act[:, cols] = (gate * jax.nn.sigmoid(gate) * up).astype(BF)
        return carry

    lax.fori_loop(0, FF // TILE, gated, 0)

    def last(n, carry):
        cols = pl.ds(pl.multiple_of(n * TILE, TILE), TILE)
        out[:, cols] = product(act[...], d_ref[:, cols]).astype(BF)
        return carry

    lax.fori_loop(0, D // TILE, last, 0, unroll=2)


def own_body(
    x, ids, gathered, bias_in, bias_out, gain, router, tokens, gates,
    w_a, w_b, hidden, squares, sems,
):
    first, second = weight_copies(gathered, w_a, w_b, sems)
    for copy in first + second:
        copy.start()
    scale = projector(x, w_a, w_b, bias_in, bias_out, hidden, tokens, squares, first, second)
    normalise(tokens, scale, gain, hidden)
    logits = product(hidden[...], router[...])
    expert = iota((ROWS, EXPERTS), 1)
    one = jnp.sum(jnp.where(expert == ids[:, 0:1], logits, 0.0), axis=1, keepdims=True)
    two = jnp.sum(jnp.where(expert == ids[:, 1:2], logits, 0.0), axis=1, keepdims=True)
    gate = jax.nn.sigmoid(one - two)
    gates[...] = jnp.where(iota((ROWS, 128), 1) == 0, gate, 1.0 - gate)


def combine_body(ids, tokens, gates, low, high, out, picks):
    expert = iota((ROWS, EXPERTS), 1)
    named = (expert == ids[:, 0:1]) | (expert == ids[:, 1:2])
    before = hot(iota((ROWS, ROWS), 1) < iota((ROWS, ROWS), 0))
    count = product(before, hot(named))
    for j in range(2):
        e = ids[:, j : j + 1]
        slot = jnp.sum(jnp.where(expert == e, count, 0.0), axis=1, keepdims=True).astype(I32)
        upper = slot >= HALF
        key = e * HALF + slot + jnp.where(upper, SLOTS - HALF, 0)
        for half in range(2):
            picks[2 * j + half] = hot(iota((ROWS, SLOTS), 1) + half * SLOTS == key)
    g0, g1 = gates[:, 0:1], gates[:, 1:2]

    def tile(n, carry):
        cols = pl.ds(pl.multiple_of(n * TILE, TILE), TILE)
        c0 = product(picks[0], low[:, cols]) + product(picks[1], high[:, cols])
        c1 = product(picks[2], low[:, cols]) + product(picks[3], high[:, cols])
        out[:, cols] = (tokens[:, cols].astype(F32) + (g0 * c0 + g1 * c1)).astype(BF)
        return carry

    lax.fori_loop(0, D // TILE, tile, 0)


def sds(shape, dtype=BF):
    return jax.ShapeDtypeStruct(shape, dtype)


def shards(
    features, token_position, expert_ids, proj_in, bias_in, proj_out, bias_out,
    norm_gain, router, w_gate, w_up, w_down,
):
    index = lambda name: lax.axis_index(name).astype(I32)
    quarter = (index("xh") * CO + index("co")).reshape(1)
    own_z = index("z").reshape(1)
    piece = call(
        piece_body, sds((PIECE, QW)), [smem(), vmem(), vmem()], vmem(), flops=10**8, name="piece"
    )(quarter, proj_in, proj_out)
    pieces = [piece] + [
        lax.ppermute(piece, "z", [(i, (i + d) % Z) for i in range(Z)]) for d in range(1, Z)
    ]
    packed = call(
        pack_body, sds((BLOCK, QW)), [smem()] + [vmem()] * Z, vmem(), flops=10**8, name="pack"
    )(own_z, *pieces)
    gathered = lax.all_gather(packed, ("xh", "xl", "y", "co"), tiled=True)

    send = call(
        send_body, sds((ROWS, SEND_W)), [vmem(), vmem()], vmem(), flops=10**9, name="send"
    )(token_position.reshape(1, ROWS), features)
    arrived = lax.all_to_all(send.reshape(EXPERTS, ROWS // EXPERTS, SEND_W), EP, 0, 0, tiled=True)
    own, blocks = call(
        place_body,
        (sds((ROWS, D_VIS)), sds((SLOTS, 2 * D_VIS))),
        [vmem(), vmem()],
        (vmem(), vmem()),
        flops=10**9,
        name="place",
    )(arrived.reshape(ROWS, SEND_W), expert_ids.T)
    received = lax.all_to_all(
        blocks.reshape(EXPERTS, HALF, 2 * D_VIS), EP, 0, 0, tiled=True
    ).reshape(SLOTS, 2 * D_VIS)

    b_in = bias_in.reshape(Z, COLUMNS, R_OUT).transpose(1, 0, 2).reshape(1, D)
    b_out = bias_out.reshape(1, D)
    gain = norm_gain.reshape(1, D)

    def expert(half):
        return pl.pallas_call(
            expert_body,
            grid=(1,),
            out_shape=sds((SLOTS, D)),
            in_specs=[pl.BlockSpec((SLOTS, D_VIS), lambda i: (0, half)), hbm()]
            + [vmem()] * 3
            + [hbm()] * 3,
            out_specs=pl.BlockSpec((SLOTS, D), lambda i: (0, 0)),
            scratch_shapes=[
                pltpu.VMEM((D_VIS, D), BF),
                pltpu.VMEM((D, D), BF),
                pltpu.VMEM((D, FF), BF),
                pltpu.VMEM((D, FF), BF),
                pltpu.VMEM((FF, D), BF),
                pltpu.VMEM((SLOTS, D), BF),
                pltpu.VMEM((SLOTS, D), BF),
                pltpu.VMEM((SLOTS, FF), BF),
                pltpu.VMEM((SLOTS, 128), F32),
                pltpu.SemaphoreType.DMA((2 * GATHERED + 3,)),
            ],
            name=f"expert{half}",
            cost_estimate=pl.CostEstimate(
                flops=2 * SLOTS * (D_VIS * D + D * D + 3 * D * FF),
                bytes_accessed=30 << 20,
                transcendentals=0,
            ),
            compiler_params=pltpu.CompilerParams(vmem_limit_bytes=52 << 20),
        )(received, gathered, b_in, b_out, gain, w_gate, w_up, w_down)

    def sent_back(outputs):
        return lax.all_to_all(
            outputs.reshape(EXPERTS, HALF, D), EP, 0, 0, tiled=True
        ).reshape(SLOTS, D)

    low = sent_back(expert(0))
    high = sent_back(expert(1))
    tokens, gates = call(
        own_body,
        (sds((ROWS, D)), sds((ROWS, 128), F32)),
        [vmem(), vmem(), hbm()] + [vmem()] * 4,
        (vmem(), vmem()),
        scratch=[
            pltpu.VMEM((D_VIS, D), BF),
            pltpu.VMEM((D, D), BF),
            pltpu.VMEM((ROWS, D), BF),
            pltpu.VMEM((ROWS, 128), F32),
            pltpu.SemaphoreType.DMA((2 * GATHERED,)),
        ],
        flops=2 * ROWS * (D_VIS * D + D * D),
        name="own",
    )(own, expert_ids, gathered, b_in, b_out, gain, router)
    return call(
        combine_body,
        sds((ROWS, D)),
        [vmem()] * 5,
        vmem(),
        scratch=[pltpu.VMEM((4, ROWS, SLOTS), BF)],
        flops=3 * 10**9,
        name="combine",
    )(expert_ids, tokens, gates, low, high)


def solution(mesh):
    fine = Mesh(mesh.devices.reshape(XH, CO, Z, XL, Y), ALL)
    rows, experts = P(ALL, None), P(EP, None, None)
    placed = (
        rows, P(ALL), rows, P(EP, None), P(), P(EP, None), P(), P(), P(),
        experts, experts, experts,
    )
    return jax.shard_map(shards, mesh=fine, in_specs=placed, out_specs=rows, check_vma=False)
```

```python
import functools

import jax
import jax.numpy as jnp
from jax import lax
from jax.experimental import pallas as pl
from jax.experimental.pallas import tpu as pltpu
from jax.sharding import Mesh, PartitionSpec as P

EPSILON = 1e-06
BF = jnp.bfloat16
F32 = jnp.float32
I32 = jnp.int32

XH, CO, Z, XL, Y = 2, 2, 8, 2, 4
ALL = ("xh", "co", "z", "xl", "y")
EP = ("z", "xl", "y")
D_VIS, D, FF = 1152, 2560, 512
ROWS, EXPERTS, CAP = 256, 64, 16
HALF = CAP // 2
SLOTS = EXPERTS * HALF
QUAD = EXPERTS * 4
UNROLL = 5
R_IN, R_OUT = D_VIS // EXPERTS, D // EXPERTS
COLUMNS = XL * Y
C_IN, C_OUT = R_IN * Z, R_OUT * Z
PIECE = 64
BLOCK = C_IN + C_OUT
QUARTERS = XH * CO
QW = D // QUARTERS
GATHERED = XH * XL * Y * CO
SEND_W = D_VIS + 128
TILE = 256


def iota(shape, dim):
    return lax.broadcasted_iota(I32, shape, dim)


def hot(mask):
    return jnp.where(mask, 1.0, 0.0).astype(BF)


def divided(x, by):
    return jnp.floor((x.astype(F32) + 0.5) * (1.0 / by)).astype(I32)


def product(a, b):
    return jnp.dot(a, b, preferred_element_type=F32)


def vmem():
    return pl.BlockSpec(memory_space=pltpu.VMEM)


def smem():
    return pl.BlockSpec(memory_space=pltpu.SMEM)


def hbm():
    return pl.BlockSpec(memory_space=pl.ANY)


def call(body, outs, in_specs, out_specs, scratch=(), flops=0, limit=48, name=None):
    return pl.pallas_call(
        body,
        out_shape=outs,
        in_specs=in_specs,
        out_specs=out_specs,
        scratch_shapes=list(scratch),
        name=name,
        cost_estimate=pl.CostEstimate(flops=flops, bytes_accessed=1 << 20, transcendentals=0),
        compiler_params=pltpu.CompilerParams(vmem_limit_bytes=limit << 20),
    )


def piece_body(quarter, w_in, w_out, piece):
    q = quarter[0]
    new = iota((1, QW), 1) + q * QW
    col = divided(new, C_OUT)
    rest = new - col * C_OUT
    z = divided(rest, R_OUT)
    old = z * (COLUMNS * R_OUT) + col * R_OUT + (rest - z * R_OUT)
    order = hot(iota((D, QW), 0) == old)
    picked = product(w_in[...], order).astype(BF)
    piece[0:R_OUT, :] = w_out[:, pl.ds(pl.multiple_of(q * QW, 128), QW)]
    piece[R_OUT : R_OUT + R_IN, :] = picked
    piece[R_OUT + R_IN : PIECE, :] = jnp.zeros((PIECE - R_OUT - R_IN, QW), BF)


def pack_body(own_z, *refs):
    pieces, out = refs[:-1], refs[-1]
    k = iota((1, PIECE), 1)
    row = iota((BLOCK, PIECE), 0)
    total = jnp.zeros((BLOCK, QW), F32)
    for d in range(Z):
        source = lax.rem(own_z[0] + (Z - d), Z)
        first = source * R_OUT + k
        second = C_OUT + source * R_IN + (k - R_OUT)
        target = jnp.where(k < R_OUT, first, jnp.where(k < R_OUT + R_IN, second, -1))
        total = total + product(hot(row == target), pieces[d][...])
    out[...] = total.astype(BF)


def send_body(position, features, out):
    pos = position[...].astype(F32)
    wide = jnp.broadcast_to(pos, (ROWS, ROWS))
    earlier = jnp.where(wide.T < wide, 1.0, 0.0)
    rank = jnp.sum(earlier, axis=0, keepdims=True)
    picks = iota((ROWS, ROWS), 0).astype(F32) == rank
    landing = pos - jnp.floor(pos * (1.0 / ROWS)) * ROWS
    landed = jnp.sum(jnp.where(picks, jnp.broadcast_to(landing, (ROWS, ROWS)), 0.0), axis=1, keepdims=True)
    ordered = product(hot(picks), features[...]).astype(BF)
    new = iota((1, D_VIS), 1)
    col = divided(new, C_IN)
    rest = new - col * C_IN
    z = divided(rest, R_IN)
    old = z * (COLUMNS * R_IN) + col * R_IN + (rest - z * R_IN)
    order = hot(iota((D_VIS, D_VIS), 0) == old)
    out[:, 0:D_VIS] = product(ordered, order).astype(BF)
    out[:, D_VIS:SEND_W] = jnp.broadcast_to(landed, (ROWS, SEND_W - D_VIS)).astype(BF)


def place_body(received, ids_t, own, blocks):
    landing = received[:, D_VIS:SEND_W].astype(F32).T[0:1, :]
    place = hot(iota((ROWS, ROWS), 0).astype(F32) == landing)
    tokens = product(place, received[:, 0:D_VIS]).astype(BF)
    own[...] = tokens
    expert = iota((EXPERTS, ROWS), 0)
    named = (expert == ids_t[0:1, :]) | (expert == ids_t[1:2, :])
    before = hot(iota((ROWS, ROWS), 0) < iota((ROWS, ROWS), 1))
    count = product(hot(named), before)
    slot = jnp.where(named, count, -1.0).astype(BF)
    spread = hot((iota((SLOTS, EXPERTS), 0) >> 3) == iota((SLOTS, EXPERTS), 1))
    slots = product(spread, slot)
    within = (iota((SLOTS, ROWS), 0) & 7).astype(F32)
    for half in range(2):
        chosen = hot(slots == within + float(half * HALF))
        blocks[:, half * D_VIS : (half + 1) * D_VIS] = product(chosen, tokens).astype(BF)


def weight_copies(gathered, w_a, w_b, sems):
    first, second = [[], []], [[], []]
    for b in range(GATHERED):
        xh, xl, y, co = b // (XL * Y * CO), b // (Y * CO) % XL, b // CO % Y, b % CO
        column, quarter = xl * Y + y, xh * CO + co
        cols = pl.ds(quarter * QW, QW)
        first[xh].append(
            pltpu.make_async_copy(
                gathered.at[pl.ds(b * BLOCK + C_OUT, C_IN), :],
                w_a.at[pl.ds(column * C_IN, C_IN), cols],
                sems.at[b],
            )
        )
        second[xh].append(
            pltpu.make_async_copy(
                gathered.at[pl.ds(b * BLOCK, C_OUT), :],
                w_b.at[pl.ds(column * C_OUT, C_OUT), cols],
                sems.at[GATHERED + b],
            )
        )
    return first, second


def started(copies):
    for copy in copies:
        copy.start()


def waited(copies):
    for copy in copies:
        copy.wait()


def gelu(pre):
    return 0.5 * pre * (1.0 + lax.erf(pre * 0.7071067811865476))


def window(n):
    return pl.ds(pl.multiple_of(n * TILE, TILE), TILE)


def projector(
    x, w_a, w_b, bias_in, bias_out, hidden, tokens, squares, first, second, third, fourth, unroll
):
    steps = D // TILE // 2

    def up(n, carry):
        cols = window(n)
        hidden[:, cols] = gelu(product(x[...], w_a[:, cols]) + bias_in[:, cols]).astype(BF)
        return carry

    def down(n, carry):
        cols = window(n)
        result = (product(hidden[...], w_b[:, cols]) + bias_out[:, cols]).astype(BF)
        tokens[:, cols] = result
        wide = result.astype(F32)
        wide = wide * wide
        squares[...] += wide[:, 0:128] + wide[:, 128:256]
        return carry

    squares[...] = jnp.zeros(squares.shape, F32)
    if unroll == 1:
        started(second[0] + second[1])
        waited(first[0] + first[1])
        lax.fori_loop(0, 2 * steps, up, 0)
        started(third + fourth)
        waited(second[0] + second[1])
        lax.fori_loop(0, 2 * steps, down, 0)
    else:
        groups = [first[0], first[1], second[0], second[1], third, fourth]
        for k, body in enumerate((up, up, down, down)):
            waited(groups[k])
            started(groups[k + 2])
            side = k % 2
            lax.fori_loop(side * steps, (side + 1) * steps, body, 0, unroll=unroll)
    mean = jnp.sum(squares[...], axis=1, keepdims=True) * (1.0 / D)
    return lax.rsqrt(mean + EPSILON)


def normalise(tokens, scale, gain, normed):
    def one(n, carry):
        cols = window(n)
        normed[:, cols] = (tokens[:, cols].astype(F32) * scale * gain[:, cols]).astype(BF)
        return carry

    lax.fori_loop(0, D // TILE, one, 0)


def expert_body(
    late, received, gathered, bias_in, bias_out, gain, w_gate, w_up, w_down, out,
    w_a, w_b, g_ref, u_ref, d_ref, x, hidden, tokens, act, squares, sems,
):
    first, second = weight_copies(gathered, w_a, w_b, sems)
    base = 2 * GATHERED
    third = [
        pltpu.make_async_copy(w_gate.at[0], g_ref, sems.at[base]),
        pltpu.make_async_copy(w_up.at[0], u_ref, sems.at[base + 1]),
    ]
    fourth = [pltpu.make_async_copy(w_down.at[0], d_ref, sems.at[base + 2])]
    started(first[0] + first[1])
    line = iota((QUAD, SLOTS), 0)
    source = (line >> 2) * HALF + (line & 3) + (4 if late else 0)
    picked = product(hot(iota((QUAD, SLOTS), 1) == source), received[:, 0:D_VIS])
    x[0:QUAD, :] = picked.astype(BF)
    if late:
        x[QUAD : QUAD + SLOTS, :] = received[:, D_VIS : 2 * D_VIS]
    scale = projector(
        x, w_a, w_b, bias_in, bias_out, hidden, tokens, squares, first, second, third, fourth,
        1 if late else UNROLL,
    )
    normalise(tokens, scale, gain, hidden)
    waited(third)

    def gated(n, carry):
        cols = window(n)
        gate = product(hidden[...], g_ref[:, cols])
        up = product(hidden[...], u_ref[:, cols])
        act[:, cols] = (gate * jax.nn.sigmoid(gate) * up).astype(BF)
        return carry

    lax.fori_loop(0, FF // TILE, gated, 0, unroll=1 if late else 2)
    waited(fourth)
    line = iota((SLOTS, QUAD), 0)
    twice = hot(iota((SLOTS, QUAD), 1) == (line >> 3) * 4 + (line & 3))
    folded = product(twice, act[0:QUAD, :]).astype(BF)
    right = (iota((SLOTS, TILE), 0) & 4) != 0
    shift = D if late else 0

    def fold(n, carry):
        low = product(folded, d_ref[:, window(n)])
        high = product(folded, d_ref[:, window(n + D // TILE // 2)])
        out[:, window(n + shift // TILE)] = jnp.where(right, high, low).astype(BF)
        return carry

    lax.fori_loop(0, D // TILE // 2, fold, 0)
    if late:

        def last(n, carry):
            cols = window(n)
            out[:, cols] = product(act[QUAD : QUAD + SLOTS, :], d_ref[:, cols]).astype(BF)
            return carry

        lax.fori_loop(0, D // TILE, last, 0)


def own_body(
    x, ids, gathered, bias_in, bias_out, gain, router, tokens, notes,
    w_a, w_b, hidden, squares, sems,
):
    first, second = weight_copies(gathered, w_a, w_b, sems)
    started(first[0] + first[1])
    scale = projector(
        x, w_a, w_b, bias_in, bias_out, hidden, tokens, squares, first, second, [], [], 1
    )
    normalise(tokens, scale, gain, hidden)
    logits = product(hidden[...], router[...])
    expert = iota((ROWS, EXPERTS), 1)
    named = (expert == ids[:, 0:1]) | (expert == ids[:, 1:2])
    before = hot(iota((ROWS, ROWS), 1) < iota((ROWS, ROWS), 0))
    count = product(before, hot(named))
    logit, key = [], []
    for j in range(2):
        e = ids[:, j : j + 1]
        logit.append(jnp.sum(jnp.where(expert == e, logits, 0.0), axis=1, keepdims=True))
        slot = jnp.sum(jnp.where(expert == e, count, 0.0), axis=1, keepdims=True)
        key.append(e.astype(F32) * CAP + slot)
    gate = jax.nn.sigmoid(logit[0] - logit[1])
    lane = iota((ROWS, 128), 1)
    notes[...] = jnp.where(
        lane == 0, gate, jnp.where(lane == 1, 1.0 - gate, jnp.where(lane == 2, key[0], key[1]))
    )


def rows_of(key, low, high, shape_rows):
    slot, expert = key & (CAP - 1), key >> 4
    return jnp.where((slot >= low) & (slot < high), expert * HALF + slot - low, shape_rows)


def pair_picks(rows):
    lane = iota((ROWS, SLOTS), 1)
    return jnp.concatenate([hot(lane == rows[0]), hot(lane == rows[1])], axis=0)


def weighed(notes, pair):
    return notes[:, 0:1] * pair[0:ROWS, :] + notes[:, 1:2] * pair[ROWS : 2 * ROWS, :]


def early_body(tokens, notes, early, partial):
    keys = [notes[:, 2 + j : 3 + j].astype(I32) for j in range(2)]
    for side in range(2):
        picks = pair_picks([rows_of(key, 0, 4, -HALF) + 4 * side for key in keys])

        def tile(n, carry):
            wide = window(n + side * (D // TILE // 2))
            pair = product(picks, early[:, window(n)])
            partial[:, wide] = tokens[:, wide].astype(F32) + weighed(notes, pair)
            return carry

        lax.fori_loop(0, D // TILE // 2, tile, 0)


def combine_body(notes, partial, late, out, folded):
    keys = [notes[:, 2 + j : 3 + j].astype(I32) for j in range(2)]
    plain = pair_picks([rows_of(key, HALF, CAP, -1) for key in keys])
    for side in range(2):
        folded[side] = pair_picks([rows_of(key, 4, HALF, -HALF) + 4 * side for key in keys])
    steps = D // TILE // 2

    def tile(n, carry):
        side = jnp.where(n >= steps, 1, 0)
        pair = product(plain, late[:, window(n)])
        pair = pair + product(folded[side], late[:, window(2 * steps + n - side * steps)])
        out[:, window(n)] = (partial[:, window(n)] + weighed(notes, pair)).astype(BF)
        return carry

    lax.fori_loop(0, 2 * steps, tile, 0, unroll=UNROLL)


def sds(shape, dtype=BF):
    return jax.ShapeDtypeStruct(shape, dtype)


def shards(
    features, token_position, expert_ids, proj_in, bias_in, proj_out, bias_out,
    norm_gain, router, w_gate, w_up, w_down,
):
    index = lambda name: lax.axis_index(name).astype(I32)
    quarter = (index("xh") * CO + index("co")).reshape(1)
    own_z = index("z").reshape(1)
    piece = call(
        piece_body, sds((PIECE, QW)), [smem(), vmem(), vmem()], vmem(), flops=10**8, name="piece"
    )(quarter, proj_in, proj_out)
    pieces = [piece] + [
        lax.ppermute(piece, "z", [(i, (i + d) % Z) for i in range(Z)]) for d in range(1, Z)
    ]
    packed = call(
        pack_body, sds((BLOCK, QW)), [smem()] + [vmem()] * Z, vmem(), flops=10**8, name="pack"
    )(own_z, *pieces)
    gathered = lax.all_gather(packed, ("xh", "xl", "y", "co"), tiled=True)

    send = call(
        send_body, sds((ROWS, SEND_W)), [vmem(), vmem()], vmem(), flops=10**9, name="send"
    )(token_position.reshape(1, ROWS), features)
    arrived = lax.all_to_all(send.reshape(EXPERTS, ROWS // EXPERTS, SEND_W), EP, 0, 0, tiled=True)
    own, blocks = call(
        place_body,
        (sds((ROWS, D_VIS)), sds((SLOTS, 2 * D_VIS))),
        [vmem(), vmem()],
        (vmem(), vmem()),
        flops=10**9,
        name="place",
    )(arrived.reshape(ROWS, SEND_W), expert_ids.T)
    received = lax.all_to_all(
        blocks.reshape(EXPERTS, HALF, 2 * D_VIS), EP, 0, 0, tiled=True
    ).reshape(SLOTS, 2 * D_VIS)

    b_in = bias_in.reshape(Z, COLUMNS, R_OUT).transpose(1, 0, 2).reshape(1, D)
    b_out = bias_out.reshape(1, D)
    gain = norm_gain.reshape(1, D)

    def expert(late):
        rows, width = (QUAD + SLOTS, D + D // 2) if late else (QUAD, D // 2)
        return call(
            functools.partial(expert_body, late),
            sds((SLOTS, width)),
            [vmem(), hbm()] + [vmem()] * 3 + [hbm()] * 3,
            vmem(),
            scratch=[
                pltpu.VMEM((D_VIS, D), BF),
                pltpu.VMEM((D, D), BF),
                pltpu.VMEM((D, FF), BF),
                pltpu.VMEM((D, FF), BF),
                pltpu.VMEM((FF, D), BF),
                pltpu.VMEM((rows, D_VIS), BF),
                pltpu.VMEM((rows, D), BF),
                pltpu.VMEM((rows, D), BF),
                pltpu.VMEM((rows, FF), BF),
                pltpu.VMEM((rows, 128), F32),
                pltpu.SemaphoreType.DMA((2 * GATHERED + 3,)),
            ],
            flops=2 * rows * (D_VIS * D + D * D + 3 * D * FF),
            limit=54,
            name="late_expert" if late else "early_expert",
        )(received, gathered, b_in, b_out, gain, w_gate, w_up, w_down)

    def sent_back(outputs):
        width = outputs.shape[1]
        return lax.all_to_all(
            outputs.reshape(EXPERTS, HALF, width), EP, 0, 0, tiled=True
        ).reshape(SLOTS, width)

    early_out = expert(False)
    early = sent_back(early_out)
    held, _ = lax.optimization_barrier((received, early_out))
    received = held
    late = sent_back(expert(True))
    tokens, notes = call(
        own_body,
        (sds((ROWS, D)), sds((ROWS, 128), F32)),
        [vmem(), vmem(), hbm()] + [vmem()] * 4,
        (vmem(), vmem()),
        scratch=[
            pltpu.VMEM((D_VIS, D), BF),
            pltpu.VMEM((D, D), BF),
            pltpu.VMEM((ROWS, D), BF),
            pltpu.VMEM((ROWS, 128), F32),
            pltpu.SemaphoreType.DMA((2 * GATHERED,)),
        ],
        flops=2 * ROWS * (D_VIS * D + D * D),
        name="own",
    )(own, expert_ids, gathered, b_in, b_out, gain, router)
    partial = call(
        early_body, sds((ROWS, D), F32), [vmem()] * 3, vmem(), flops=10**9, name="early_combine"
    )(tokens, notes, early)
    return call(
        combine_body, sds((ROWS, D)), [vmem()] * 3, vmem(),
        scratch=[pltpu.VMEM((2, 2 * ROWS, SLOTS), BF)], flops=3 * 10**9, name="combine",
    )(notes, partial, late)


def solution(mesh):
    fine = Mesh(mesh.devices.reshape(XH, CO, Z, XL, Y), ALL)
    rows, experts = P(ALL, None), P(EP, None, None)
    placed = (
        rows, P(ALL), rows, P(EP, None), P(), P(EP, None), P(), P(), P(),
        experts, experts, experts,
    )
    return jax.shard_map(shards, mesh=fine, in_specs=placed, out_specs=rows, check_vma=False)
```

```python
import functools

import jax
import jax.numpy as jnp
from jax import lax
from jax.experimental import pallas as pl
from jax.experimental.pallas import tpu as pltpu
from jax.sharding import Mesh, PartitionSpec as P

EPSILON = 1e-06
BF = jnp.bfloat16
F32 = jnp.float32
I32 = jnp.int32

XH, CO, Z, XL, Y = 2, 2, 8, 2, 4
ALL = ("xh", "co", "z", "xl", "y")
EP = ("z", "xl", "y")
D_VIS, D, FF = 1152, 2560, 512
ROWS, EXPERTS, CAP = 256, 64, 16
HALF = CAP // 2
SLOTS = EXPERTS * HALF
QUAD = EXPERTS * 4
UNROLL = 5
R_IN, R_OUT = D_VIS // EXPERTS, D // EXPERTS
COLUMNS = XL * Y
C_IN, C_OUT = R_IN * Z, R_OUT * Z
PIECE = 64
BLOCK = C_IN + C_OUT
QUARTERS = XH * CO
QW = D // QUARTERS
GATHERED = XH * XL * Y * CO
SEND_W = D_VIS + 128
TILE = 256


def iota(shape, dim):
    return lax.broadcasted_iota(I32, shape, dim)


def hot(mask):
    return jnp.where(mask, 1.0, 0.0).astype(BF)


def divided(x, by):
    return jnp.floor((x.astype(F32) + 0.5) * (1.0 / by)).astype(I32)


def product(a, b):
    return jnp.dot(a, b, preferred_element_type=F32)


def vmem():
    return pl.BlockSpec(memory_space=pltpu.VMEM)


def smem():
    return pl.BlockSpec(memory_space=pltpu.SMEM)


def hbm():
    return pl.BlockSpec(memory_space=pl.ANY)


def call(body, outs, in_specs, out_specs, scratch=(), flops=0, limit=48, name=None):
    return pl.pallas_call(
        body,
        out_shape=outs,
        in_specs=in_specs,
        out_specs=out_specs,
        scratch_shapes=list(scratch),
        name=name,
        cost_estimate=pl.CostEstimate(flops=flops, bytes_accessed=1 << 20, transcendentals=0),
        compiler_params=pltpu.CompilerParams(vmem_limit_bytes=limit << 20),
    )


def piece_body(quarter, w_in, w_out, piece):
    q = quarter[0]
    new = iota((1, QW), 1) + q * QW
    col = divided(new, C_OUT)
    rest = new - col * C_OUT
    z = divided(rest, R_OUT)
    old = z * (COLUMNS * R_OUT) + col * R_OUT + (rest - z * R_OUT)
    order = hot(iota((D, QW), 0) == old)
    picked = product(w_in[...], order).astype(BF)
    piece[0:R_OUT, :] = w_out[:, pl.ds(pl.multiple_of(q * QW, 128), QW)]
    piece[R_OUT : R_OUT + R_IN, :] = picked
    piece[R_OUT + R_IN : PIECE, :] = jnp.zeros((PIECE - R_OUT - R_IN, QW), BF)


def pack_body(own_z, *refs):
    pieces, out, stack = refs[:Z], refs[Z], refs[Z + 1]
    for d in range(Z):
        stack[d * PIECE : (d + 1) * PIECE, :] = pieces[d][...]
    lane = iota((1, Z * PIECE), 1)
    source, k = (own_z[0] + (Z - (lane >> 6))) & (Z - 1), lane & (PIECE - 1)
    first = source * R_OUT + k
    second = C_OUT + source * R_IN + (k - R_OUT)
    target = jnp.where(k < R_OUT, first, jnp.where(k < R_OUT + R_IN, second, -1))
    order = hot(iota((BLOCK, Z * PIECE), 0) == target)
    out[...] = product(order, stack[...]).astype(BF)


def send_body(position, features, out):
    pos = position[...].astype(F32)
    wide = jnp.broadcast_to(pos, (ROWS, ROWS))
    earlier = jnp.where(wide.T < wide, 1.0, 0.0)
    rank = jnp.sum(earlier, axis=0, keepdims=True)
    picks = iota((ROWS, ROWS), 0).astype(F32) == rank
    landing = pos - jnp.floor(pos * (1.0 / ROWS)) * ROWS
    landed = jnp.sum(jnp.where(picks, jnp.broadcast_to(landing, (ROWS, ROWS)), 0.0), axis=1, keepdims=True)
    ordered = product(hot(picks), features[...]).astype(BF)
    new = iota((1, D_VIS), 1)
    col = divided(new, C_IN)
    rest = new - col * C_IN
    z = divided(rest, R_IN)
    old = z * (COLUMNS * R_IN) + col * R_IN + (rest - z * R_IN)
    order = hot(iota((D_VIS, D_VIS), 0) == old)
    out[:, 0:D_VIS] = product(ordered, order).astype(BF)
    out[:, D_VIS:SEND_W] = jnp.broadcast_to(landed, (ROWS, SEND_W - D_VIS)).astype(BF)


def place_body(received, ids_t, own, blocks):
    landing = received[:, D_VIS:SEND_W].astype(F32).T[0:1, :]
    place = hot(iota((ROWS, ROWS), 0).astype(F32) == landing)
    tokens = product(place, received[:, 0:D_VIS]).astype(BF)
    own[...] = tokens
    expert = iota((EXPERTS, ROWS), 0)
    named = (expert == ids_t[0:1, :]) | (expert == ids_t[1:2, :])
    before = hot(iota((ROWS, ROWS), 0) < iota((ROWS, ROWS), 1))
    count = product(hot(named), before)
    slot = jnp.where(named, count, -1.0).astype(BF)
    spread = hot((iota((SLOTS, EXPERTS), 0) >> 3) == iota((SLOTS, EXPERTS), 1))
    slots = product(spread, slot)
    within = (iota((SLOTS, ROWS), 0) & 7).astype(F32)
    for half in range(2):
        chosen = hot(slots == within + float(half * HALF))
        blocks[:, half * D_VIS : (half + 1) * D_VIS] = product(chosen, tokens).astype(BF)


def weight_copies(gathered, w_a, w_b, sems):
    first, second = [[], []], [[], []]
    for b in range(GATHERED):
        xh, xl, y, co = b // (XL * Y * CO), b // (Y * CO) % XL, b // CO % Y, b % CO
        column, quarter = xl * Y + y, xh * CO + co
        cols = pl.ds(quarter * QW, QW)
        first[xh].append(
            pltpu.make_async_copy(
                gathered.at[pl.ds(b * BLOCK + C_OUT, C_IN), :],
                w_a.at[pl.ds(column * C_IN, C_IN), cols],
                sems.at[b],
            )
        )
        second[xh].append(
            pltpu.make_async_copy(
                gathered.at[pl.ds(b * BLOCK, C_OUT), :],
                w_b.at[pl.ds(column * C_OUT, C_OUT), cols],
                sems.at[GATHERED + b],
            )
        )
    return first, second


def started(copies):
    for copy in copies:
        copy.start()


def waited(copies):
    for copy in copies:
        copy.wait()


def gelu(pre):
    return 0.5 * pre * (1.0 + lax.erf(pre * 0.7071067811865476))


def window(n):
    return pl.ds(pl.multiple_of(n * TILE, TILE), TILE)


def projector(
    x, w_a, w_b, bias_in, bias_out, hidden, tokens, squares, first, second, third, fourth, unroll
):
    steps = D // TILE // 2

    def up(n, carry):
        cols = window(n)
        hidden[:, cols] = gelu(product(x[...], w_a[:, cols]) + bias_in[:, cols]).astype(BF)
        return carry

    def down(n, carry):
        cols = window(n)
        result = (product(hidden[...], w_b[:, cols]) + bias_out[:, cols]).astype(BF)
        tokens[:, cols] = result
        wide = result.astype(F32)
        wide = wide * wide
        squares[...] += wide[:, 0:128] + wide[:, 128:256]
        return carry

    squares[...] = jnp.zeros(squares.shape, F32)
    if unroll == 1:
        waited(first[0] + first[1])
        started(second[0] + second[1])
        lax.fori_loop(0, 2 * steps, up, 0)
        waited(second[0] + second[1])
        started(third + fourth)
        lax.fori_loop(0, 2 * steps, down, 0)
    else:
        groups = [first[0], first[1], second[0], second[1], third, fourth]
        for k, body in enumerate((up, up, down, down)):
            waited(groups[k])
            started(groups[k + 2])
            side = k % 2
            lax.fori_loop(side * steps, (side + 1) * steps, body, 0, unroll=unroll)
    mean = jnp.sum(squares[...], axis=1, keepdims=True) * (1.0 / D)
    return lax.rsqrt(mean + EPSILON)


def normalise(tokens, scale, gain, normed):
    def one(n, carry):
        cols = window(n)
        normed[:, cols] = (tokens[:, cols].astype(F32) * scale * gain[:, cols]).astype(BF)
        return carry

    lax.fori_loop(0, D // TILE, one, 0)


def pick_body(received, early, late):
    line, lane = iota((QUAD, SLOTS), 0), iota((QUAD, SLOTS), 1)
    row = (line >> 2) * HALF + (line & 3)
    first = received[:, 0:D_VIS]
    early[...] = product(hot(lane == row), first).astype(BF)
    late[0:QUAD, :] = product(hot(lane == row + 4), first).astype(BF)
    late[QUAD : QUAD + SLOTS, :] = received[:, D_VIS : 2 * D_VIS]


def expert_body(
    late, rows_in, gathered, bias_in, bias_out, gain, w_gate, w_up, w_down, out,
    w_a, w_b, g_ref, u_ref, d_ref, x, hidden, tokens, act, squares, sems,
):
    first, second = weight_copies(gathered, w_a, w_b, sems)
    base = 2 * GATHERED
    third = [
        pltpu.make_async_copy(w_gate.at[0], g_ref, sems.at[base]),
        pltpu.make_async_copy(w_up.at[0], u_ref, sems.at[base + 1]),
    ]
    fourth = [pltpu.make_async_copy(w_down.at[0], d_ref, sems.at[base + 2])]
    first[0].append(pltpu.make_async_copy(rows_in, x, sems.at[base + 3]))
    started(first[0] + first[1])
    unroll = 1 if late else UNROLL
    scale = projector(
        x, w_a, w_b, bias_in, bias_out, hidden, tokens, squares, first, second, third, fourth,
        unroll,
    )
    normalise(tokens, scale, gain, hidden)
    waited(third)

    def gated(n, carry):
        cols = window(n)
        gate = product(hidden[...], g_ref[:, cols])
        up = product(hidden[...], u_ref[:, cols])
        act[:, cols] = (gate * jax.nn.sigmoid(gate) * up).astype(BF)
        return carry

    lax.fori_loop(0, FF // TILE, gated, 0, unroll=1 if late else 2)
    waited(fourth)
    line = iota((SLOTS, QUAD), 0)
    twice = hot(iota((SLOTS, QUAD), 1) == (line >> 3) * 4 + (line & 3))
    folded = product(twice, act[0:QUAD, :]).astype(BF)
    right = (iota((SLOTS, TILE), 0) & 4) != 0
    shift = D // TILE if late else 0

    def fold(n, carry):
        low = product(folded, d_ref[:, window(n)])
        high = product(folded, d_ref[:, window(n + D // TILE // 2)])
        out[:, window(n + shift)] = jnp.where(right, high, low).astype(BF)
        return carry

    lax.fori_loop(0, D // TILE // 2, fold, 0, unroll=unroll)
    if late:

        def plain(n, carry):
            cols = window(n)
            out[:, cols] = product(act[QUAD : QUAD + SLOTS, :], d_ref[:, cols]).astype(BF)
            return carry

        lax.fori_loop(0, D // TILE, plain, 0)


def own_body(
    x, ids, gathered, bias_in, bias_out, gain, router, tokens, notes,
    w_a, w_b, hidden, squares, sems,
):
    first, second = weight_copies(gathered, w_a, w_b, sems)
    started(first[0] + first[1])
    scale = projector(
        x, w_a, w_b, bias_in, bias_out, hidden, tokens, squares, first, second, [], [], 1
    )
    normalise(tokens, scale, gain, hidden)
    logits = product(hidden[...], router[...])
    expert = iota((ROWS, EXPERTS), 1)
    named = (expert == ids[:, 0:1]) | (expert == ids[:, 1:2])
    before = hot(iota((ROWS, ROWS), 1) < iota((ROWS, ROWS), 0))
    count = product(before, hot(named))
    logit, key = [], []
    for j in range(2):
        e = ids[:, j : j + 1]
        logit.append(jnp.sum(jnp.where(expert == e, logits, 0.0), axis=1, keepdims=True))
        slot = jnp.sum(jnp.where(expert == e, count, 0.0), axis=1, keepdims=True)
        key.append(e.astype(F32) * CAP + slot)
    gate = jax.nn.sigmoid(logit[0] - logit[1])
    lane = iota((ROWS, 128), 1)
    notes[...] = jnp.where(
        lane == 0, gate, jnp.where(lane == 1, 1.0 - gate, jnp.where(lane == 2, key[0], key[1]))
    )


def rows_of(key, low, high, shape_rows):
    slot, expert = key & (CAP - 1), key >> 4
    return jnp.where((slot >= low) & (slot < high), expert * HALF + slot - low, shape_rows)


def pair_picks(rows, count):
    lane = iota((ROWS, count), 1)
    return jnp.concatenate([hot(lane == rows[0]), hot(lane == rows[1])], axis=0)


def weighed(notes, pair):
    return notes[:, 0:1] * pair[0:ROWS, :] + notes[:, 1:2] * pair[ROWS : 2 * ROWS, :]


def keys_of(notes):
    return [notes[:, 2 + j : 3 + j].astype(I32) for j in range(2)]


def early_body(tokens, notes, early, partial, plain, folded):
    keys = keys_of(notes)
    plain[...] = pair_picks([rows_of(key, HALF, CAP, -1) for key in keys], SLOTS)
    for side in range(2):
        lines = [rows_of(key, 4, HALF, -HALF) + 4 * side for key in keys]
        folded[side] = pair_picks(lines, SLOTS)
    for side in range(2):
        picks = pair_picks([rows_of(key, 0, 4, -HALF) + 4 * side for key in keys], SLOTS)

        def tile(n, carry):
            wide = window(n + side * (D // TILE // 2))
            pair = product(picks, early[:, window(n)])
            partial[:, wide] = tokens[:, wide].astype(F32) + weighed(notes, pair)
            return carry

        lax.fori_loop(0, D // TILE // 2, tile, 0)


def combine_body(notes, partial, late, late_fold, plain, folded, out):
    pair = product(plain[...], late[...]) + product(folded[0], late_fold[...])
    out[...] = (partial[...] + weighed(notes, pair)).astype(BF)


def sds(shape, dtype=BF):
    return jax.ShapeDtypeStruct(shape, dtype)


def shards(
    features, token_position, expert_ids, proj_in, bias_in, proj_out, bias_out,
    norm_gain, router, w_gate, w_up, w_down,
):
    index = lambda name: lax.axis_index(name).astype(I32)
    quarter = (index("xh") * CO + index("co")).reshape(1)
    own_z = index("z").reshape(1)
    piece = call(
        piece_body, sds((PIECE, QW)), [smem(), vmem(), vmem()], vmem(), flops=10**8, name="piece"
    )(quarter, proj_in, proj_out)
    pieces = [piece] + [
        lax.ppermute(piece, "z", [(i, (i + d) % Z) for i in range(Z)]) for d in range(1, Z)
    ]
    packed = call(
        pack_body, sds((BLOCK, QW)), [smem()] + [vmem()] * Z, vmem(),
        scratch=[pltpu.VMEM((Z * PIECE, QW), BF)], flops=10**8, name="pack",
    )(own_z, *pieces)
    gathered = lax.all_gather(packed, ("xh", "xl", "y", "co"), tiled=True)

    send = call(
        send_body, sds((ROWS, SEND_W)), [vmem(), vmem()], vmem(), flops=10**9, name="send"
    )(token_position.reshape(1, ROWS), features)
    arrived = lax.all_to_all(send.reshape(EXPERTS, ROWS // EXPERTS, SEND_W), EP, 0, 0, tiled=True)
    own, blocks = call(
        place_body,
        (sds((ROWS, D_VIS)), sds((SLOTS, 2 * D_VIS))),
        [vmem(), vmem()],
        (vmem(), vmem()),
        flops=10**9,
        name="place",
    )(arrived.reshape(ROWS, SEND_W), expert_ids.T)
    received = lax.all_to_all(
        blocks.reshape(EXPERTS, HALF, 2 * D_VIS), EP, 0, 0, tiled=True
    ).reshape(SLOTS, 2 * D_VIS)

    b_in = bias_in.reshape(Z, COLUMNS, R_OUT).transpose(1, 0, 2).reshape(1, D)
    b_out = bias_out.reshape(1, D)
    gain = norm_gain.reshape(1, D)

    early_x, late_x = call(
        pick_body,
        (sds((QUAD, D_VIS)), sds((QUAD + SLOTS, D_VIS))),
        [vmem()],
        (vmem(), vmem()),
        flops=10**9,
        name="pick",
    )(received)

    def expert(late, x):
        rows = x.shape[0]
        return call(
            functools.partial(expert_body, late),
            sds((SLOTS, D + D // 2 if late else D // 2)),
            [hbm(), hbm()] + [vmem()] * 3 + [hbm()] * 3,
            vmem(),
            scratch=[
                pltpu.VMEM((D_VIS, D), BF),
                pltpu.VMEM((D, D), BF),
                pltpu.VMEM((D, FF), BF),
                pltpu.VMEM((D, FF), BF),
                pltpu.VMEM((FF, D), BF),
                pltpu.VMEM((rows, D_VIS), BF),
                pltpu.VMEM((rows, D), BF),
                pltpu.VMEM((rows, D), BF),
                pltpu.VMEM((rows, FF), BF),
                pltpu.VMEM((rows, 128), F32),
                pltpu.SemaphoreType.DMA((2 * GATHERED + 4,)),
            ],
            flops=2 * rows * (D_VIS * D + D * D + 3 * D * FF),
            limit=59,
            name="late_expert" if late else "early_expert",
        )(x, gathered, b_in, b_out, gain, w_gate, w_up, w_down)

    def sent_back(outputs):
        width = outputs.shape[1]
        return lax.all_to_all(
            outputs.reshape(EXPERTS, HALF, width), EP, 0, 0, tiled=True
        ).reshape(SLOTS, width)

    early_out = expert(False, early_x)
    early = sent_back(early_out)
    late_x, _ = lax.optimization_barrier((late_x, early_out))
    late = sent_back(expert(True, late_x))
    tokens, notes = call(
        own_body,
        (sds((ROWS, D)), sds((ROWS, 128), F32)),
        [vmem(), vmem(), hbm()] + [vmem()] * 4,
        (vmem(), vmem()),
        scratch=[
            pltpu.VMEM((D_VIS, D), BF),
            pltpu.VMEM((D, D), BF),
            pltpu.VMEM((ROWS, D), BF),
            pltpu.VMEM((ROWS, 128), F32),
            pltpu.SemaphoreType.DMA((2 * GATHERED,)),
        ],
        flops=2 * ROWS * (D_VIS * D + D * D),
        name="own",
    )(own, expert_ids, gathered, b_in, b_out, gain, router)
    picks = (sds((2 * ROWS, SLOTS)), sds((2, 2 * ROWS, SLOTS)))
    partial, plain, folded = call(
        early_body,
        (sds((ROWS, D), F32), *picks),
        [vmem()] * 3,
        (vmem(),) * 3,
        flops=10**9,
        name="early_combine",
    )(tokens, notes, early)
    steps = D // (D // 2)
    return pl.pallas_call(
        combine_body,
        grid=(steps,),
        out_shape=sds((ROWS, D)),
        in_specs=[
            pl.BlockSpec((ROWS, 128), lambda n: (0, 0)),
            pl.BlockSpec((ROWS, (D // 2)), lambda n: (0, n)),
            pl.BlockSpec((SLOTS, (D // 2)), lambda n: (0, n)),
            pl.BlockSpec((SLOTS, (D // 2)), lambda n: (0, steps + n % (steps // 2))),
            pl.BlockSpec((2 * ROWS, SLOTS), lambda n: (0, 0)),
            pl.BlockSpec((1, 2 * ROWS, SLOTS), lambda n: (n // (steps // 2), 0, 0)),
        ],
        out_specs=pl.BlockSpec((ROWS, (D // 2)), lambda n: (0, n)),
        name="combine",
        cost_estimate=pl.CostEstimate(flops=3 * 10**9, bytes_accessed=8 << 20, transcendentals=0),
        compiler_params=pltpu.CompilerParams(vmem_limit_bytes=60 << 20),
    )(notes, partial, late, late, plain, folded)


def solution(mesh):
    fine = Mesh(mesh.devices.reshape(XH, CO, Z, XL, Y), ALL)
    rows, experts = P(ALL, None), P(EP, None, None)
    placed = (
        rows, P(ALL), rows, P(EP, None), P(), P(EP, None), P(), P(), P(),
        experts, experts, experts,
    )
    return jax.shard_map(shards, mesh=fine, in_specs=placed, out_specs=rows, check_vma=False)
```

```python
import functools

import jax
import jax.numpy as jnp
from jax import lax
from jax.experimental import pallas as pl
from jax.experimental.pallas import tpu as pltpu
from jax.sharding import Mesh, PartitionSpec as P

EPSILON = 1e-06
BF = jnp.bfloat16
F32 = jnp.float32
I32 = jnp.int32

XH, CO, Z, XL, Y = 2, 2, 8, 2, 4
ALL = ("xh", "co", "z", "xl", "y")
EP = ("z", "xl", "y")
D_VIS, D, FF = 1152, 2560, 512
ROWS, EXPERTS, CAP = 256, 64, 16
HALF = CAP // 2
SLOTS = EXPERTS * HALF
QUAD = EXPERTS * 4
UNROLL = 5
R_IN, R_OUT = D_VIS // EXPERTS, D // EXPERTS
COLUMNS = XL * Y
C_IN, C_OUT = R_IN * Z, R_OUT * Z
PIECE = 64
BLOCK = C_IN + C_OUT
QUARTERS = XH * CO
QW = D // QUARTERS
GATHERED = XH * XL * Y * CO
SEND_W = D_VIS + 128
TILE = 256


def iota(shape, dim):
    return lax.broadcasted_iota(I32, shape, dim)


def hot(mask):
    return jnp.where(mask, 1.0, 0.0).astype(BF)


def divided(x, by):
    return jnp.floor((x.astype(F32) + 0.5) * (1.0 / by)).astype(I32)


def product(a, b):
    return jnp.dot(a, b, preferred_element_type=F32)


def vmem():
    return pl.BlockSpec(memory_space=pltpu.VMEM)


def smem():
    return pl.BlockSpec(memory_space=pltpu.SMEM)


def hbm():
    return pl.BlockSpec(memory_space=pl.ANY)


def call(body, outs, in_specs, out_specs, scratch=(), flops=0, limit=48, name=None):
    return pl.pallas_call(
        body,
        out_shape=outs,
        in_specs=in_specs,
        out_specs=out_specs,
        scratch_shapes=list(scratch),
        name=name,
        cost_estimate=pl.CostEstimate(flops=flops, bytes_accessed=1 << 20, transcendentals=0),
        compiler_params=pltpu.CompilerParams(vmem_limit_bytes=limit << 20),
    )


def piece_body(quarter, w_in, w_out, piece):
    q = quarter[0]
    new = iota((1, QW), 1) + q * QW
    col = divided(new, C_OUT)
    rest = new - col * C_OUT
    z = divided(rest, R_OUT)
    old = z * (COLUMNS * R_OUT) + col * R_OUT + (rest - z * R_OUT)
    order = hot(iota((D, QW), 0) == old)
    picked = product(w_in[...], order).astype(BF)
    piece[0:R_OUT, :] = w_out[:, pl.ds(pl.multiple_of(q * QW, 128), QW)]
    piece[R_OUT : R_OUT + R_IN, :] = picked
    piece[R_OUT + R_IN : PIECE, :] = jnp.zeros((PIECE - R_OUT - R_IN, QW), BF)


def pack_body(own_z, *refs):
    pieces, out, stack = refs[:Z], refs[Z], refs[Z + 1]
    for d in range(Z):
        stack[d * PIECE : (d + 1) * PIECE, :] = pieces[d][...]
    lane = iota((1, Z * PIECE), 1)
    source, k = (own_z[0] + (Z - (lane >> 6))) & (Z - 1), lane & (PIECE - 1)
    first = source * R_OUT + k
    second = C_OUT + source * R_IN + (k - R_OUT)
    target = jnp.where(k < R_OUT, first, jnp.where(k < R_OUT + R_IN, second, -1))
    order = hot(iota((BLOCK, Z * PIECE), 0) == target)
    out[...] = product(order, stack[...]).astype(BF)


def send_body(position, features, out):
    pos = position[...].astype(F32)
    wide = jnp.broadcast_to(pos, (ROWS, ROWS))
    earlier = jnp.where(wide.T < wide, 1.0, 0.0)
    rank = jnp.sum(earlier, axis=0, keepdims=True)
    picks = iota((ROWS, ROWS), 0).astype(F32) == rank
    landing = pos - jnp.floor(pos * (1.0 / ROWS)) * ROWS
    landed = jnp.sum(jnp.where(picks, jnp.broadcast_to(landing, (ROWS, ROWS)), 0.0), axis=1, keepdims=True)
    ordered = product(hot(picks), features[...]).astype(BF)
    new = iota((1, D_VIS), 1)
    col = divided(new, C_IN)
    rest = new - col * C_IN
    z = divided(rest, R_IN)
    old = z * (COLUMNS * R_IN) + col * R_IN + (rest - z * R_IN)
    order = hot(iota((D_VIS, D_VIS), 0) == old)
    out[:, 0:D_VIS] = product(ordered, order).astype(BF)
    out[:, D_VIS:SEND_W] = jnp.broadcast_to(landed, (ROWS, SEND_W - D_VIS)).astype(BF)


def place_body(received, ids_t, own, blocks):
    landing = received[:, D_VIS:SEND_W].astype(F32).T[0:1, :]
    place = hot(iota((ROWS, ROWS), 0).astype(F32) == landing)
    tokens = product(place, received[:, 0:D_VIS]).astype(BF)
    own[...] = tokens
    expert = iota((EXPERTS, ROWS), 0)
    named = (expert == ids_t[0:1, :]) | (expert == ids_t[1:2, :])
    before = hot(iota((ROWS, ROWS), 0) < iota((ROWS, ROWS), 1))
    count = product(hot(named), before)
    slot = jnp.where(named, count, -1.0).astype(BF)
    spread = hot((iota((SLOTS, EXPERTS), 0) >> 3) == iota((SLOTS, EXPERTS), 1))
    slots = product(spread, slot)
    within = (iota((SLOTS, ROWS), 0) & 7).astype(F32)
    for half in range(2):
        chosen = hot(slots == within + float(half * HALF))
        blocks[:, half * D_VIS : (half + 1) * D_VIS] = product(chosen, tokens).astype(BF)


def weight_copies(gathered, w_a, w_b, sems):
    first, second = [[], []], [[], []]
    for b in range(GATHERED):
        xh, xl, y, co = b // (XL * Y * CO), b // (Y * CO) % XL, b // CO % Y, b % CO
        column, quarter = xl * Y + y, xh * CO + co
        cols = pl.ds(quarter * QW, QW)
        first[xh].append(
            pltpu.make_async_copy(
                gathered.at[pl.ds(b * BLOCK + C_OUT, C_IN), :],
                w_a.at[pl.ds(column * C_IN, C_IN), cols],
                sems.at[b],
            )
        )
        second[xh].append(
            pltpu.make_async_copy(
                gathered.at[pl.ds(b * BLOCK, C_OUT), :],
                w_b.at[pl.ds(column * C_OUT, C_OUT), cols],
                sems.at[GATHERED + b],
            )
        )
    return first, second


def started(copies):
    for copy in copies:
        copy.start()


def waited(copies):
    for copy in copies:
        copy.wait()


def gelu(pre):
    return 0.5 * pre * (1.0 + lax.erf(pre * 0.7071067811865476))


def window(n):
    return pl.ds(pl.multiple_of(n * TILE, TILE), TILE)


def projector(
    x, w_a, w_b, bias_in, bias_out, hidden, tokens, squares, first, second, third, fourth, unroll
):
    steps = D // TILE // 2

    def up(n, carry):
        cols = window(n)
        hidden[:, cols] = gelu(product(x[...], w_a[:, cols]) + bias_in[:, cols]).astype(BF)
        return carry

    def down(n, carry):
        cols = window(n)
        result = (product(hidden[...], w_b[:, cols]) + bias_out[:, cols]).astype(BF)
        tokens[:, cols] = result
        wide = result.astype(F32)
        wide = wide * wide
        squares[...] += wide[:, 0:128] + wide[:, 128:256]
        return carry

    squares[...] = jnp.zeros(squares.shape, F32)
    if unroll == 1:
        started(second[0])
        waited(first[0] + first[1])
        started(second[1])
        lax.fori_loop(0, 2 * steps, up, 0, unroll=2 if x.shape[0] > ROWS else 1)
        waited(second[0] + second[1])
        started(third + fourth)
        lax.fori_loop(0, 2 * steps, down, 0)
    else:
        groups = [first[0], first[1], second[0], second[1], third, fourth]
        for k, body in enumerate((up, up, down, down)):
            waited(groups[k])
            started(groups[k + 2])
            side = k % 2
            lax.fori_loop(side * steps, (side + 1) * steps, body, 0, unroll=unroll)
    mean = jnp.sum(squares[...], axis=1, keepdims=True) * (1.0 / D)
    return lax.rsqrt(mean + EPSILON)


def normalise(tokens, scale, gain, normed):
    def one(n, carry):
        cols = window(n)
        normed[:, cols] = (tokens[:, cols].astype(F32) * scale * gain[:, cols]).astype(BF)
        return carry

    lax.fori_loop(0, D // TILE, one, 0)


def pick_body(received, early, late):
    line, lane = iota((QUAD, SLOTS), 0), iota((QUAD, SLOTS), 1)
    row = (line >> 2) * HALF + (line & 3)
    first = received[:, 0:D_VIS]
    early[...] = product(hot(lane == row), first).astype(BF)
    late[0:QUAD, :] = product(hot(lane == row + 4), first).astype(BF)
    late[QUAD : QUAD + SLOTS, :] = received[:, D_VIS : 2 * D_VIS]


def expert_body(
    late, rows_in, gathered, bias_in, bias_out, gain, w_gate, w_up, w_down, out,
    w_a, w_b, g_ref, u_ref, d_ref, x, hidden, tokens, act, squares, sems,
):
    first, second = weight_copies(gathered, w_a, w_b, sems)
    base = 2 * GATHERED
    third = [
        pltpu.make_async_copy(w_gate.at[0], g_ref, sems.at[base]),
        pltpu.make_async_copy(w_up.at[0], u_ref, sems.at[base + 1]),
    ]
    fourth = [pltpu.make_async_copy(w_down.at[0], d_ref, sems.at[base + 2])]
    first[0].append(pltpu.make_async_copy(rows_in, x, sems.at[base + 3]))
    started(first[0] + first[1])
    unroll = 1 if late else UNROLL
    scale = projector(
        x, w_a, w_b, bias_in, bias_out, hidden, tokens, squares, first, second, third, fourth,
        unroll,
    )
    normalise(tokens, scale, gain, hidden)
    waited(third)

    def gated(n, carry):
        cols = window(n)
        gate = product(hidden[...], g_ref[:, cols])
        up = product(hidden[...], u_ref[:, cols])
        act[:, cols] = (gate * jax.nn.sigmoid(gate) * up).astype(BF)
        return carry

    lax.fori_loop(0, FF // TILE, gated, 0, unroll=1 if late else 2)
    waited(fourth)
    line = iota((SLOTS, QUAD), 0)
    twice = hot(iota((SLOTS, QUAD), 1) == (line >> 3) * 4 + (line & 3))
    folded = product(twice, act[0:QUAD, :]).astype(BF)
    right = (iota((SLOTS, TILE), 0) & 4) != 0
    shift = D // TILE if late else 0

    def fold(n, carry):
        low = product(folded, d_ref[:, window(n)])
        high = product(folded, d_ref[:, window(n + D // TILE // 2)])
        out[:, window(n + shift)] = jnp.where(right, high, low).astype(BF)
        return carry

    lax.fori_loop(0, D // TILE // 2, fold, 0, unroll=unroll)
    if late:

        def plain(n, carry):
            cols = window(n)
            out[:, cols] = product(act[QUAD : QUAD + SLOTS, :], d_ref[:, cols]).astype(BF)
            return carry

        lax.fori_loop(0, D // TILE, plain, 0)


def own_body(
    x, ids, gathered, bias_in, bias_out, gain, router, tokens, notes,
    w_a, w_b, hidden, squares, sems,
):
    first, second = weight_copies(gathered, w_a, w_b, sems)
    started(first[0] + first[1])
    scale = projector(
        x, w_a, w_b, bias_in, bias_out, hidden, tokens, squares, first, second, [], [], 1
    )
    normalise(tokens, scale, gain, hidden)
    logits = product(hidden[...], router[...])
    expert = iota((ROWS, EXPERTS), 1)
    named = (expert == ids[:, 0:1]) | (expert == ids[:, 1:2])
    before = hot(iota((ROWS, ROWS), 1) < iota((ROWS, ROWS), 0))
    count = product(before, hot(named))
    logit, key = [], []
    for j in range(2):
        e = ids[:, j : j + 1]
        logit.append(jnp.sum(jnp.where(expert == e, logits, 0.0), axis=1, keepdims=True))
        slot = jnp.sum(jnp.where(expert == e, count, 0.0), axis=1, keepdims=True)
        key.append(e.astype(F32) * CAP + slot)
    gate = jax.nn.sigmoid(logit[0] - logit[1])
    lane = iota((ROWS, 128), 1)
    notes[...] = jnp.where(
        lane == 0, gate, jnp.where(lane == 1, 1.0 - gate, jnp.where(lane == 2, key[0], key[1]))
    )


def rows_of(key, low, high, shape_rows):
    slot, expert = key & (CAP - 1), key >> 4
    return jnp.where((slot >= low) & (slot < high), expert * HALF + slot - low, shape_rows)


def pair_picks(rows, count):
    lane = iota((ROWS, count), 1)
    return jnp.concatenate([hot(lane == rows[0]), hot(lane == rows[1])], axis=0)


def weighed(notes, pair):
    return notes[:, 0:1] * pair[0:ROWS, :] + notes[:, 1:2] * pair[ROWS : 2 * ROWS, :]


def keys_of(notes):
    return [notes[:, 2 + j : 3 + j].astype(I32) for j in range(2)]


def early_body(tokens, notes, early, partial, plain, folded):
    keys = keys_of(notes)
    plain[...] = pair_picks([rows_of(key, HALF, CAP, -1) for key in keys], SLOTS)
    for side in range(2):
        lines = [rows_of(key, 4, HALF, -HALF) + 4 * side for key in keys]
        folded[side] = pair_picks(lines, SLOTS)
    for side in range(2):
        picks = pair_picks([rows_of(key, 0, 4, -HALF) + 4 * side for key in keys], SLOTS)

        def tile(n, carry):
            wide = window(n + side * (D // TILE // 2))
            pair = product(picks, early[:, window(n)])
            partial[:, wide] = tokens[:, wide].astype(F32) + weighed(notes, pair)
            return carry

        lax.fori_loop(0, D // TILE // 2, tile, 0)


def combine_body(notes, partial, late, late_fold, plain, folded, out):
    pair = product(plain[...], late[...]) + product(folded[0], late_fold[...])
    out[...] = (partial[...] + weighed(notes, pair)).astype(BF)


def sds(shape, dtype=BF):
    return jax.ShapeDtypeStruct(shape, dtype)


def shards(
    features, token_position, expert_ids, proj_in, bias_in, proj_out, bias_out,
    norm_gain, router, w_gate, w_up, w_down,
):
    index = lambda name: lax.axis_index(name).astype(I32)
    quarter = (index("xh") * CO + index("co")).reshape(1)
    own_z = index("z").reshape(1)
    piece = call(
        piece_body, sds((PIECE, QW)), [smem(), vmem(), vmem()], vmem(), flops=10**8, name="piece"
    )(quarter, proj_in, proj_out)
    pieces = [piece] + [
        lax.ppermute(piece, "z", [(i, (i + d) % Z) for i in range(Z)]) for d in range(1, Z)
    ]
    packed = call(
        pack_body, sds((BLOCK, QW)), [smem()] + [vmem()] * Z, vmem(),
        scratch=[pltpu.VMEM((Z * PIECE, QW), BF)], flops=10**8, name="pack",
    )(own_z, *pieces)
    gathered = lax.all_gather(packed, ("xh", "xl", "y", "co"), tiled=True)

    send = call(
        send_body, sds((ROWS, SEND_W)), [vmem(), vmem()], vmem(), flops=10**9, name="send"
    )(token_position.reshape(1, ROWS), features)
    arrived = lax.all_to_all(send.reshape(EXPERTS, ROWS // EXPERTS, SEND_W), EP, 0, 0, tiled=True)
    own, blocks = call(
        place_body,
        (sds((ROWS, D_VIS)), sds((SLOTS, 2 * D_VIS))),
        [vmem(), vmem()],
        (vmem(), vmem()),
        flops=10**9,
        name="place",
    )(arrived.reshape(ROWS, SEND_W), expert_ids.T)
    received = lax.all_to_all(
        blocks.reshape(EXPERTS, HALF, 2 * D_VIS), EP, 0, 0, tiled=True
    ).reshape(SLOTS, 2 * D_VIS)

    b_in = bias_in.reshape(Z, COLUMNS, R_OUT).transpose(1, 0, 2).reshape(1, D)
    b_out = bias_out.reshape(1, D)
    gain = norm_gain.reshape(1, D)

    early_x, late_x = call(
        pick_body,
        (sds((QUAD, D_VIS)), sds((QUAD + SLOTS, D_VIS))),
        [vmem()],
        (vmem(), vmem()),
        flops=10**9,
        name="pick",
    )(received)

    def expert(late, x):
        rows = x.shape[0]
        return call(
            functools.partial(expert_body, late),
            sds((SLOTS, D + D // 2 if late else D // 2)),
            [hbm(), hbm()] + [vmem()] * 3 + [hbm()] * 3,
            vmem(),
            scratch=[
                pltpu.VMEM((D_VIS, D), BF),
                pltpu.VMEM((D, D), BF),
                pltpu.VMEM((D, FF), BF),
                pltpu.VMEM((D, FF), BF),
                pltpu.VMEM((FF, D), BF),
                pltpu.VMEM((rows, D_VIS), BF),
                pltpu.VMEM((rows, D), BF),
                pltpu.VMEM((rows, D), BF),
                pltpu.VMEM((rows, FF), BF),
                pltpu.VMEM((rows, 128), F32),
                pltpu.SemaphoreType.DMA((2 * GATHERED + 4,)),
            ],
            flops=2 * rows * (D_VIS * D + D * D + 3 * D * FF),
            limit=59,
            name="late_expert" if late else "early_expert",
        )(x, gathered, b_in, b_out, gain, w_gate, w_up, w_down)

    def sent_back(outputs):
        width = outputs.shape[1]
        return lax.all_to_all(
            outputs.reshape(EXPERTS, HALF, width), EP, 0, 0, tiled=True
        ).reshape(SLOTS, width)

    early_out = expert(False, early_x)
    early = sent_back(early_out)
    late_x, _ = lax.optimization_barrier((late_x, early_out))
    late = sent_back(expert(True, late_x))
    tokens, notes = call(
        own_body,
        (sds((ROWS, D)), sds((ROWS, 128), F32)),
        [vmem(), vmem(), hbm()] + [vmem()] * 4,
        (vmem(), vmem()),
        scratch=[
            pltpu.VMEM((D_VIS, D), BF),
            pltpu.VMEM((D, D), BF),
            pltpu.VMEM((ROWS, D), BF),
            pltpu.VMEM((ROWS, 128), F32),
            pltpu.SemaphoreType.DMA((2 * GATHERED,)),
        ],
        flops=2 * ROWS * (D_VIS * D + D * D),
        name="own",
    )(own, expert_ids, gathered, b_in, b_out, gain, router)
    picks = (sds((2 * ROWS, SLOTS)), sds((2, 2 * ROWS, SLOTS)))
    partial, plain, folded = call(
        early_body,
        (sds((ROWS, D), F32), *picks),
        [vmem()] * 3,
        (vmem(),) * 3,
        flops=10**9,
        name="early_combine",
    )(tokens, notes, early)
    steps = D // (D // 2)
    return pl.pallas_call(
        combine_body,
        grid=(steps,),
        out_shape=sds((ROWS, D)),
        in_specs=[
            pl.BlockSpec((ROWS, 128), lambda n: (0, 0)),
            pl.BlockSpec((ROWS, (D // 2)), lambda n: (0, n)),
            pl.BlockSpec((SLOTS, (D // 2)), lambda n: (0, n)),
            pl.BlockSpec((SLOTS, (D // 2)), lambda n: (0, steps + n % (steps // 2))),
            pl.BlockSpec((2 * ROWS, SLOTS), lambda n: (0, 0)),
            pl.BlockSpec((1, 2 * ROWS, SLOTS), lambda n: (n // (steps // 2), 0, 0)),
        ],
        out_specs=pl.BlockSpec((ROWS, (D // 2)), lambda n: (0, n)),
        name="combine",
        cost_estimate=pl.CostEstimate(flops=3 * 10**9, bytes_accessed=8 << 20, transcendentals=0),
        compiler_params=pltpu.CompilerParams(vmem_limit_bytes=60 << 20),
    )(notes, partial, late, late, plain, folded)


def solution(mesh):
    fine = Mesh(mesh.devices.reshape(XH, CO, Z, XL, Y), ALL)
    rows, experts = P(ALL, None), P(EP, None, None)
    placed = (
        rows, P(ALL), rows, P(EP, None), P(), P(EP, None), P(), P(), P(),
        experts, experts, experts,
    )
    return jax.shard_map(shards, mesh=fine, in_specs=placed, out_specs=rows, check_vma=False)
```
